32 devices in a mesh: pair: 2 (over y), dp: 8 (over z, x), ep: 2 (over core).
Axes of the slice: x: 2, y: 2, z: 4, core: 2. Of those that a mesh axis runs over, the one named last changes fastest.
Arguments:
- activations: bfloat16 [12288, 1024], P(('pair', 'dp'), 'ep'), parts along dimension 1, may hold values from -6 to 6
- cotangents: bfloat16 [12288, 4096], P(('pair', 'dp'), 'ep'), parts along dimension 1, may hold values from -0.875 to 0.875
Outputs:
- averaged_grad: bfloat16 [512, 4096], P('pair', 'ep'), parts along dimension 1
The draws below stay inside these ranges and needn't reach their ends.
There are 2 independent parts, one for each index of `ep`. The reference program is written for one: setup_inputs(seed, part) draws one part's arguments, and reference() takes and returns one part's arrays. A program takes and returns all parts, laid end to end along the dimension named above; each array names one. Nothing has to cross between parts.
All inputs are finite; a program needn't handle non-finite values.
Results may differ from the reference program's by a relative error of at most 0.001.
Values may be sent and summed in bfloat16 or wider, within the bound.
A program may use at most 64 MiB of HBM per device.

```python
import jax
import jax.numpy as jnp

FF = 2048
ROWS = 512
TOK_DEV = 768
REPLICAS = 16
TOKENS = 12288
N_PAIR = 2
N_DP = 8


def raised(drawn, stream_key, source, target, parts, factor):
    def block_of(position):
        return (jnp.arange(drawn.shape[position]) // (drawn.shape[position] // parts)).reshape((-1,) + (1,) * (drawn.ndim - 1 - position))

    near = jax.random.permutation(stream_key, parts)[block_of(target)]
    second = (block_of(target) + parts // 2) % parts
    return jnp.where((block_of(source) == near) | (block_of(source) == second), factor * drawn, drawn)


def steps_of(own_key, extent, cuts, least, largest):
    def one(position, parts):
        draws = jax.random.uniform(jax.random.fold_in(jax.random.fold_in(own_key, 6), position), (parts,), jnp.float32, least / len(cuts), largest / len(cuts))
        return jnp.repeat(jnp.exp(draws), extent[position] // parts).reshape((-1,) + (1,) * (len(extent) - position - 1))

    factor_of = one(*cuts[0])
    for cut in cuts[1:]:
        factor_of = factor_of * one(*cut)
    return factor_of


def scatter_about(key, shape, scale, bound, cuts=(), held_as=jnp.bfloat16):
    entries = jax.random.normal(key, shape, jnp.float32) * scale
    if len(cuts) > 0:
        entries = steps_of(key, shape, cuts, -0.22, 0.18) * entries
    return jnp.clip(entries, min=-bound, max=bound).astype(held_as)


def gaussian_with(own_key, dims, scale, limit, cuts, heavy, held_as=jnp.bfloat16):
    drawn = scale * jax.random.normal(own_key, dims, jnp.float32)
    if cuts:
        drawn = drawn * steps_of(own_key, dims, cuts, -0.22, 0.18)
    return jnp.clip(raised(drawn, jax.random.fold_in(own_key, 3), *heavy), -limit, limit).astype(held_as)


def setup_inputs(seed: int = 0, part: int = 0) -> dict:
    keys = jax.random.split(jax.random.key(seed), 3)
    part_keys = jax.random.split(jax.random.fold_in(keys[2], part), 3)
    return {
        "activations": gaussian_with(part_keys[0], (TOKENS, ROWS), 1.0, 6.0, ((0, 16),), (0, 1, 16, 2.0)),
        "cotangents": scatter_about(part_keys[1], (TOKENS, FF), (max(1, TOK_DEV // (N_PAIR * N_DP))) ** -0.5, 0.875, ((0, 16),)),
    }


def reference(activations, cotangents):
    grad_sum = jnp.dot(activations.T, cotangents, preferred_element_type=jnp.float32)
    return (grad_sum / REPLICAS).astype(jnp.bfloat16)
```

```python
import functools

import jax
import jax.numpy as jnp
from jax import lax
from jax.experimental import pallas as pl
from jax.experimental.pallas import tpu as pltpu
from jax.sharding import PartitionSpec as P

LANES = 128
SPLIT = 2
AHEAD = 4
CROSS = 4


def kernel(np_, nx, nz, nc, ns, act_ref, cot_ref, out_ref, act_t, part, f1, f2, zr,
           s1, r1, s2, r2, sz, rz, sg, rg, sx, rx):
    p = lax.axis_index("pair")
    dp = lax.axis_index("dp")
    z, x = dp // nx, dp % nx
    rs = part.shape[-2]
    chunks = nc * ns
    rows_p = nz * ns * rs
    cols_x = nc * LANES

    def other(i, q, n):
        return lax.rem(i + q, n)

    def to_pair(q):
        return {"pair": other(p, q, np_)}

    def to_x(q):
        return {"dp": z * nx + other(x, q, nx)}

    def to_z(q):
        return {"dp": other(z, q, nz) * nx + x}

    def crossed(k):
        return lax.rem(k // ns, CROSS) == CROSS - 1

    def remote(src, dst, ssem, rsem, peer):
        return pltpu.make_async_remote_copy(
            src_ref=src, dst_ref=dst, send_sem=ssem, recv_sem=rsem,
            device_id=peer, device_id_type=pl.DeviceIdType.MESH)

    def first_a(k, q):
        return remote(part.at[k, other(p, q, np_)], f1.at[k, pl.ds(p * nx, nx)],
                      s1.at[k, q], r1.at[k, p], to_pair(q))

    def first_b(k, q):
        return remote(part.at[k, :, other(x, q, nx)], f1.at[k, pl.ds(x * np_, np_)],
                      s1.at[k, q], r1.at[k, x], to_x(q))

    def second_a(k, q):
        return remote(part.at[k, p, other(x, q, nx)], f2.at[k, x], s2.at[k, q], r2.at[k, x], to_x(q))

    def second_b(k, q):
        return remote(part.at[k, other(p, q, np_), x], f2.at[k, p], s2.at[k, q], r2.at[k, p], to_pair(q))

    def along_z(k, q):
        return remote(part.at[k, p, x, other(z, q, nz)], zr.at[k, z], sz.at[k, q], rz.at[k, z], to_z(q))

    def piece(k, zi, xi):
        c, s = k // ns, lax.rem(k, ns)
        row = pl.multiple_of((zi * ns + s) * rs, rs)
        col = pl.multiple_of(xi * cols_x + c * LANES, LANES)
        return out_ref.at[pl.ds(row, rs), pl.ds(col, LANES)]

    def gather_z(k, q):
        here = piece(k, z, x)
        return remote(here, here, sg.at[k, q], rg.at[k, z], to_z(q))

    def gather_x(k, zo, q):
        zi = other(z, zo, nz)
        here = piece(k, zi, x)
        return remote(here, here, sx.at[k, zi, q], rx.at[k, zi, x], to_x(q))

    def arrived(dst, ssem, rsem):
        remote(dst, dst, ssem, rsem, to_pair(1)).wait_recv()

    def start_first(k):
        @pl.when(crossed(k))
        def _():
            for q in range(1, nx):
                first_b(k, q).start()

        @pl.when(jnp.logical_not(crossed(k)))
        def _():
            for q in range(1, np_):
                first_a(k, q).start()

    def stage2(k):
        @pl.when(jnp.logical_not(crossed(k)))
        def _():
            for q in range(1, np_):
                o = other(p, q, np_)
                arrived(f1.at[k, pl.ds(o * nx, nx)], s1.at[k, q], r1.at[k, o])
                for i in range(nx):
                    part[k, p, i] += f1[k, o * nx + i]
            for q in range(1, nx):
                second_a(k, q).start()

        @pl.when(crossed(k))
        def _():
            for q in range(1, nx):
                o = other(x, q, nx)
                arrived(f1.at[k, pl.ds(o * np_, np_)], s1.at[k, q], r1.at[k, o])
                for i in range(np_):
                    part[k, i, x] += f1[k, o * np_ + i]
            for q in range(1, np_):
                second_b(k, q).start()

    def stage3(k):
        @pl.when(jnp.logical_not(crossed(k)))
        def _():
            for q in range(1, nx):
                o = other(x, q, nx)
                arrived(f2.at[k, o], s2.at[k, q], r2.at[k, o])
                part[k, p, x] += f2[k, o]

        @pl.when(crossed(k))
        def _():
            for q in range(1, np_):
                o = other(p, q, np_)
                arrived(f2.at[k, o], s2.at[k, q], r2.at[k, o])
                part[k, p, x] += f2[k, o]

        for q in range(1, nz):
            along_z(k, q).start()

    def stage4(k):
        total = part[k, p, x, z]
        for q in range(1, nz):
            o = other(z, q, nz)
            arrived(zr.at[k, o], sz.at[k, q], rz.at[k, o])
            total = total + zr[k, o]
        replicas = np_ * nx * nz
        piece(k, z, x)[...] = (total / replicas).astype(out_ref.dtype)
        for q in range(1, nz):
            gather_z(k, q).start()
        for q in range(1, nx):
            gather_x(k, 0, q).start()

    def stage5(k):
        for zo in range(1, nz):
            o = other(z, zo, nz)
            arrived(piece(k, o, x), sg.at[k, zo], rg.at[k, o])
            for q in range(1, nx):
                gather_x(k, zo, q).start()

    def stage6(k):
        for zi in range(nz):
            for q in range(1, nx):
                o = other(x, q, nx)
                arrived(piece(k, zi, o), sx.at[k, zi, q], rx.at[k, zi, o])

    def finish(k):
        @pl.when(jnp.logical_not(crossed(k)))
        def _():
            for q in range(1, np_):
                first_a(k, q).wait_send()
            for q in range(1, nx):
                second_a(k, q).wait_send()

        @pl.when(crossed(k))
        def _():
            for q in range(1, nx):
                first_b(k, q).wait_send()
            for q in range(1, np_):
                second_b(k, q).wait_send()

        for q in range(1, nz):
            along_z(k, q).wait_send()
            gather_z(k, q).wait_send()
        for zo in range(nz):
            for q in range(1, nx):
                gather_x(k, zo, q).wait_send()

    barrier = pltpu.get_barrier_semaphore()
    peers = [to_pair(q) for q in range(1, np_)] + [to_x(q) for q in range(1, nx)] + [to_z(q) for q in range(1, nz)]
    for peer in peers:
        pl.semaphore_signal(barrier, inc=1, device_id=peer, device_id_type=pl.DeviceIdType.MESH)

    act_t[...] = act_ref[...].T

    def compute(c):
        for xi in range(nx):
            col = pl.multiple_of(xi * cols_x + c * LANES, LANES)
            grad = jnp.dot(act_t[...], cot_ref[:, pl.ds(col, LANES)], preferred_element_type=jnp.float32)
            for pi in range(np_):
                for zi in range(nz):
                    for s in range(ns):
                        row = pi * rows_p + (zi * ns + s) * rs
                        part[c * ns + s, pi, xi, zi] = grad[row:row + rs]

    compute(0)
    pl.semaphore_wait(barrier, len(peers))
    ahead = min(AHEAD, chunks)

    def send_ready(c):
        for s in range(ns):
            k = c * ns + s
            pl.when(k < ahead)(functools.partial(start_first, k))

    send_ready(0)

    @pl.loop(1, nc)
    def _(c):
        compute(c)
        send_ready(c)

    @pl.loop(0, chunks + 3)
    def _(t):
        pl.when(t + ahead < chunks)(lambda: start_first(t + ahead))
        pl.when(t < chunks)(lambda: stage2(t))
        pl.when((t >= 1) & (t - 1 < chunks))(lambda: stage3(t - 1))
        pl.when((t >= 2) & (t - 2 < chunks))(lambda: stage4(t - 2))
        pl.when(t >= 3)(lambda: stage5(t - 3))

    @pl.loop(0, chunks)
    def _(k):
        stage6(k)
        finish(k)


def solution(mesh):
    np_, ndp = mesh.shape["pair"], mesh.shape["dp"]
    nx = 1
    while (2 * nx) ** 2 <= ndp and ndp % (2 * nx) == 0:
        nx *= 2
    nz = ndp // nx

    def local(activations, cotangents):
        rows, cols = activations.shape[1], cotangents.shape[1]
        nc = cols // nx // LANES
        ns = SPLIT
        rs = rows // np_ // nz // ns
        chunks = nc * ns
        wide = max(np_, nx)
        f32 = jnp.float32
        dma = pltpu.SemaphoreType.DMA
        return pl.pallas_call(
            functools.partial(kernel, np_, nx, nz, nc, ns),
            out_shape=jax.ShapeDtypeStruct((rows // np_, cols), jnp.bfloat16),
            in_specs=[pl.BlockSpec(memory_space=pltpu.VMEM)] * 2,
            out_specs=pl.BlockSpec(memory_space=pltpu.VMEM),
            scratch_shapes=[
                pltpu.VMEM((rows, activations.shape[0]), activations.dtype),
                pltpu.VMEM((chunks, np_, nx, nz, rs, LANES), f32),
                pltpu.VMEM((chunks, np_ * nx, nz, rs, LANES), f32),
                pltpu.VMEM((chunks, wide, nz, rs, LANES), f32),
                pltpu.VMEM((chunks, nz, rs, LANES), f32),
                dma((chunks, wide)), dma((chunks, wide)),
                dma((chunks, wide)), dma((chunks, wide)),
                dma((chunks, nz)), dma((chunks, nz)),
                dma((chunks, nz)), dma((chunks, nz)),
                dma((chunks, nz, nx)), dma((chunks, nz, nx)),
            ],
            compiler_params=pltpu.CompilerParams(
                collective_id=0, has_side_effects=True, vmem_limit_bytes=60 * 1024 * 1024),
        )(activations, cotangents)

    in_specs = (P(("pair", "dp"), "ep"), P(("pair", "dp"), "ep"))
    return jax.shard_map(local, mesh=mesh, in_specs=in_specs, out_specs=P("pair", "ep"), check_vma=False)
```

```python
import functools

import jax
import jax.numpy as jnp
from jax import lax
from jax.experimental import pallas as pl
from jax.experimental.pallas import tpu as pltpu
from jax.sharding import PartitionSpec as P

LANES = 128
SPLIT = 2
AHEAD = 3
CROSS = 2
LAG = (4, 7, 10)


def kernel(np_, nx, nz, nc, ns, act_hbm, cot_hbm, out_ref, act_ref, cot_ref, act_t, part, f1, f2, zr,
           s1, r1, s2, r2, sz, rz, sg, rg, sx, rx, load):
    p = lax.axis_index("pair")
    dp = lax.axis_index("dp")
    z, x = dp // nx, dp % nx
    rs = part.shape[-2]
    chunks = nc * ns
    rows_p = nz * ns * rs
    cols_x = nc * LANES

    def other(i, q, n):
        return lax.rem(i + q, n)

    def to_pair(q):
        return {"pair": other(p, q, np_)}

    def to_x(q):
        return {"dp": z * nx + other(x, q, nx)}

    def to_z(q):
        return {"dp": other(z, q, nz) * nx + x}

    def crossed(k):
        return lax.rem(k, CROSS) == CROSS - 1

    def remote(src, dst, ssem, rsem, peer):
        return pltpu.make_async_remote_copy(
            src_ref=src, dst_ref=dst, send_sem=ssem, recv_sem=rsem,
            device_id=peer, device_id_type=pl.DeviceIdType.MESH)

    def first_a(k, q):
        return remote(part.at[k, other(p, q, np_)], f1.at[k, pl.ds(p * nx, nx)],
                      s1.at[k, q], r1.at[k, p], to_pair(q))

    def first_b(k, q):
        return remote(part.at[k, :, other(x, q, nx)], f1.at[k, pl.ds(x * np_, np_)],
                      s1.at[k, q], r1.at[k, x], to_x(q))

    def second_a(k, q):
        return remote(part.at[k, p, other(x, q, nx)], f2.at[k, x], s2.at[k, q], r2.at[k, x], to_x(q))

    def second_b(k, q):
        return remote(part.at[k, other(p, q, np_), x], f2.at[k, p], s2.at[k, q], r2.at[k, p], to_pair(q))

    def along_z(k, q):
        return remote(part.at[k, p, x, other(z, q, nz)], zr.at[k, z], sz.at[k, q], rz.at[k, z], to_z(q))

    def piece(k, zi, xi):
        c, s = k // ns, lax.rem(k, ns)
        row = pl.multiple_of((zi * ns + s) * rs, rs)
        col = pl.multiple_of(xi * cols_x + c * LANES, LANES)
        return out_ref.at[pl.ds(row, rs), pl.ds(col, LANES)]

    def gather_z(k, q):
        here = piece(k, z, x)
        return remote(here, here, sg.at[k, q], rg.at[k, z], to_z(q))

    def gather_x(k, zo, q):
        zi = other(z, zo, nz)
        here = piece(k, zi, x)
        return remote(here, here, sx.at[k, zi, q], rx.at[k, zi, x], to_x(q))

    def arrived(dst, ssem, rsem):
        remote(dst, dst, ssem, rsem, to_pair(1)).wait_recv()

    def start_first(k):
        @pl.when(crossed(k))
        def _():
            for q in range(1, nx):
                first_b(k, q).start()

        @pl.when(jnp.logical_not(crossed(k)))
        def _():
            for q in range(1, np_):
                first_a(k, q).start()

    def stage2(k):
        @pl.when(jnp.logical_not(crossed(k)))
        def _():
            for q in range(1, np_):
                o = other(p, q, np_)
                arrived(f1.at[k, pl.ds(o * nx, nx)], s1.at[k, q], r1.at[k, o])
                for i in range(nx):
                    part[k, p, i] += f1[k, o * nx + i]
            for q in range(1, nx):
                second_a(k, q).start()

        @pl.when(crossed(k))
        def _():
            for q in range(1, nx):
                o = other(x, q, nx)
                arrived(f1.at[k, pl.ds(o * np_, np_)], s1.at[k, q], r1.at[k, o])
                for i in range(np_):
                    part[k, i, x] += f1[k, o * np_ + i]
            for q in range(1, np_):
                second_b(k, q).start()

    def stage3(k):
        @pl.when(jnp.logical_not(crossed(k)))
        def _():
            for q in range(1, nx):
                o = other(x, q, nx)
                arrived(f2.at[k, o], s2.at[k, q], r2.at[k, o])
                part[k, p, x] += f2[k, o]

        @pl.when(crossed(k))
        def _():
            for q in range(1, np_):
                o = other(p, q, np_)
                arrived(f2.at[k, o], s2.at[k, q], r2.at[k, o])
                part[k, p, x] += f2[k, o]

        for q in range(1, nz):
            along_z(k, q).start()

    def stage4(k):
        total = part[k, p, x, z]
        for q in range(1, nz):
            o = other(z, q, nz)
            arrived(zr.at[k, o], sz.at[k, q], rz.at[k, o])
            total = total + zr[k, o]
        replicas = np_ * nx * nz
        piece(k, z, x)[...] = (total / replicas).astype(out_ref.dtype)
        for q in range(1, nz):
            gather_z(k, q).start()
        for q in range(1, nx):
            gather_x(k, 0, q).start()

    def stage5(k):
        for zo in range(1, nz):
            o = other(z, zo, nz)
            arrived(piece(k, o, x), sg.at[k, zo], rg.at[k, o])
            for q in range(1, nx):
                gather_x(k, zo, q).start()

    def stage6(k):
        for zi in range(nz):
            for q in range(1, nx):
                o = other(x, q, nx)
                arrived(piece(k, zi, o), sx.at[k, zi, q], rx.at[k, zi, o])

    def finish(k):
        @pl.when(jnp.logical_not(crossed(k)))
        def _():
            for q in range(1, np_):
                first_a(k, q).wait_send()
            for q in range(1, nx):
                second_a(k, q).wait_send()

        @pl.when(crossed(k))
        def _():
            for q in range(1, nx):
                first_b(k, q).wait_send()
            for q in range(1, np_):
                second_b(k, q).wait_send()

        for q in range(1, nz):
            along_z(k, q).wait_send()
            gather_z(k, q).wait_send()
        for zo in range(nz):
            for q in range(1, nx):
                gather_x(k, zo, q).wait_send()

    barrier = pltpu.get_barrier_semaphore()
    peers = [to_pair(q) for q in range(1, np_)] + [to_x(q) for q in range(1, nx)] + [to_z(q) for q in range(1, nz)]
    for peer in peers:
        pl.semaphore_signal(barrier, inc=1, device_id=peer, device_id_type=pl.DeviceIdType.MESH)

    loads = [pltpu.make_async_copy(act_hbm, act_ref, load.at[0]), pltpu.make_async_copy(cot_hbm, cot_ref, load.at[1])]
    for copy in loads:
        copy.start()
    loads[0].wait()
    act_t[...] = act_ref[...].T
    loads[1].wait()
    width = 2 if nc % 2 == 0 else 1

    @pl.loop(0, nc // width)
    def _(g):
        for xi in range(nx):
            col = pl.multiple_of(xi * cols_x + g * (width * LANES), LANES)
            grad = jnp.dot(act_t[...], cot_ref[:, pl.ds(col, width * LANES)], preferred_element_type=jnp.float32)
            for w in range(width):
                for pi in range(np_):
                    for zi in range(nz):
                        for s in range(ns):
                            row = pi * rows_p + (zi * ns + s) * rs
                            part[(g * width + w) * ns + s, pi, xi, zi] = grad[row:row + rs, w * LANES:(w + 1) * LANES]

    pl.semaphore_wait(barrier, len(peers))
    ahead = min(AHEAD, chunks)
    for k in range(ahead):
        start_first(k)

    @pl.loop(0, chunks + LAG[2])
    def _(t):
        pl.when(t + ahead < chunks)(lambda: start_first(t + ahead))
        pl.when(t < chunks)(lambda: stage2(t))
        pl.when((t >= LAG[0]) & (t - LAG[0] < chunks))(lambda: stage3(t - LAG[0]))
        pl.when((t >= LAG[1]) & (t - LAG[1] < chunks))(lambda: stage4(t - LAG[1]))
        pl.when(t >= LAG[2])(lambda: stage5(t - LAG[2]))

    @pl.loop(0, chunks)
    def _(k):
        stage6(k)
        finish(k)


def solution(mesh):
    np_, ndp = mesh.shape["pair"], mesh.shape["dp"]
    nx = 1
    while (2 * nx) ** 2 <= ndp and ndp % (2 * nx) == 0:
        nx *= 2
    nz = ndp // nx

    def local(activations, cotangents):
        rows, cols = activations.shape[1], cotangents.shape[1]
        nc = cols // nx // LANES
        ns = SPLIT
        rs = rows // np_ // nz // ns
        chunks = nc * ns
        wide = max(np_, nx)
        f32 = jnp.float32
        dma = pltpu.SemaphoreType.DMA
        return pl.pallas_call(
            functools.partial(kernel, np_, nx, nz, nc, ns),
            out_shape=jax.ShapeDtypeStruct((rows // np_, cols), jnp.bfloat16),
            in_specs=[pl.BlockSpec(memory_space=pltpu.HBM)] * 2,
            out_specs=pl.BlockSpec(memory_space=pltpu.VMEM),
            scratch_shapes=[
                pltpu.VMEM(activations.shape, activations.dtype),
                pltpu.VMEM(cotangents.shape, cotangents.dtype),
                pltpu.VMEM((rows, activations.shape[0]), activations.dtype),
                pltpu.VMEM((chunks, np_, nx, nz, rs, LANES), f32),
                pltpu.VMEM((chunks, np_ * nx, nz, rs, LANES), f32),
                pltpu.VMEM((chunks, wide, nz, rs, LANES), f32),
                pltpu.VMEM((chunks, nz, rs, LANES), f32),
                dma((chunks, wide)), dma((chunks, wide)),
                dma((chunks, wide)), dma((chunks, wide)),
                dma((chunks, nz)), dma((chunks, nz)),
                dma((chunks, nz)), dma((chunks, nz)),
                dma((chunks, nz, nx)), dma((chunks, nz, nx)),
                dma((2,)),
            ],
            compiler_params=pltpu.CompilerParams(
                collective_id=0, has_side_effects=True, vmem_limit_bytes=60 * 1024 * 1024),
        )(activations, cotangents)

    in_specs = (P(("pair", "dp"), "ep"), P(("pair", "dp"), "ep"))
    return jax.shard_map(local, mesh=mesh, in_specs=in_specs, out_specs=P("pair", "ep"), check_vma=False)
```
